512 devices in a mesh: row: 16 (over x, y_lo), col: 32 (over y_hi, z, core).
Axes of the slice: x: 4, y: 8 (y_hi: 2, y_lo: 4; y = y_hi * 4 + y_lo), z: 8, core: 2. Of those that a mesh axis runs over, the one named last changes fastest.
Arguments:
- queries: bfloat16 [2048, 4096], P(('row', 'col')), may hold values from -4 to 4
- documents: bfloat16 [4096, 4096], P(('row', 'col')), may hold values from -4 to 4
- positive: int32 [2048], P(('row', 'col')), may hold values from 0 to 4095, as said below
Outputs:
- mean_loss: float32 [], replicated
- query_grad: bfloat16 [2048, 4096], P(('row', 'col'))
- document_grad: bfloat16 [4096, 4096], P(('row', 'col'))
The draws below stay inside these ranges and needn't reach their ends.
Inputs may be any that keep to these rules, and one draw needn't show every extreme that they name: `positive`: the 2048 entries are distinct document indices.
All inputs are finite; a program needn't handle non-finite values.
Results may differ from the reference program's by a relative error of at most 0.02.
Values may be sent and summed in bfloat16 or wider, within the bound.
A program may use at most 64 MiB of HBM per device.

```python
import math
import jax
import jax.numpy as jnp
from jax import lax

D = 4096
LEVELS = 4
Q_DEV = 4
DOC_DEV = 8
QUERIES = 2048
DOCS = 4096
N_ROW = 16
N_COL = 32


def paired_draw(key):
    keys = jax.random.split(jax.random.fold_in(key, 101), 2)
    pairing = draw_positive(key, 0)
    steps = jnp.arange(QUERIES, dtype=jnp.float32) / (QUERIES - 1)
    query_vals = jnp.clip(jax.random.normal(keys[0], (QUERIES, D)), -4.0, 4.0)
    doc_vals = jax.random.normal(keys[1], (DOCS, D))
    rising = (1.0 + 3.0 * steps) / math.sqrt(D)
    doc_vals = doc_vals.at[pairing].add(rising[:, None] * query_vals)
    doc_vals = jnp.clip(doc_vals, -4.0, 4.0)
    return (query_vals.astype(jnp.float32), doc_vals.astype(jnp.float32))


def draw_queries(key, part):
    return paired_draw(key)[0].astype(jnp.bfloat16)


def draw_documents(key, part):
    return paired_draw(key)[1].astype(jnp.bfloat16)


def draw_positive(key, part):
    keys = jax.random.split(jax.random.fold_in(key, 211), 2)
    middle = 1 + jax.random.permutation(keys[0], DOCS - 2)[:QUERIES - 2]
    chosen = jnp.concatenate([jnp.array([0, DOCS - 1], jnp.int32), middle.astype(jnp.int32)])
    return jax.random.permutation(keys[1], chosen).astype(jnp.int32)


def setup_inputs(seed: int = 0) -> dict:
    key_list = jax.random.split(jax.random.key(seed), 4)
    return {
        "queries": draw_queries(jax.random.fold_in(key_list[3], 71), 0),
        "documents": draw_documents(jax.random.fold_in(key_list[3], 71), 0),
        "positive": draw_positive(jax.random.fold_in(key_list[3], 71), 0),
    }


def reference(queries, documents, positive):
    onehot = (jnp.arange(DOCS, dtype=jnp.int32)[None, :] == positive[:, None].astype(jnp.int32)).astype(jnp.float32)
    loss_total = jnp.zeros((), jnp.float32)
    grads = []
    for level_index in range(LEVELS):
        narrow = D >> level_index
        inv_temp = 4.0 / math.sqrt(narrow)
        logits = lax.dot_general(queries[:, :narrow], documents[:, :narrow], (((1,), (1,)), ((), ())), preferred_element_type=jnp.float32) * inv_temp
        largest = lax.optimization_barrier(jnp.max(logits, axis=1, keepdims=True))
        lse = largest[:, 0] + jnp.log(lax.optimization_barrier(jnp.sum(jnp.exp(logits - largest), axis=1)))
        picked = jnp.take_along_axis(logits, positive[:, None].astype(jnp.int32), axis=1)[:, 0]
        loss_total = loss_total + jnp.sum(lse - picked)
        grads.append((jnp.exp(logits - lse[:, None]) - onehot).astype(jnp.bfloat16))
    mean_loss = loss_total / (QUERIES * LEVELS)
    grad_blocks = [grad.reshape(QUERIES, N_ROW, N_COL, DOC_DEV) for grad in grads]
    doc_cols = documents.reshape(N_ROW, N_COL, DOC_DEV, D)

    def query_step(index, running):
        part_docs = lax.dynamic_index_in_dim(doc_cols, index, 1, keepdims=False).reshape(N_ROW * DOC_DEV, D)
        partial_value = jnp.zeros((QUERIES, D), jnp.float32)
        for level_index in range(LEVELS):
            narrow = D >> level_index
            part_grad = lax.dynamic_index_in_dim(grad_blocks[level_index], index, 2, keepdims=False).reshape(QUERIES, N_ROW * DOC_DEV)
            contrib = jnp.dot(part_grad, part_docs[:, :narrow], preferred_element_type=jnp.float32) * math.sqrt(D / narrow)
            partial_value = partial_value + jnp.pad(contrib, ((0, 0), (0, D - narrow)))
        partial_value = partial_value.astype(jnp.bfloat16)
        partial_value = lax.optimization_barrier(partial_value)
        return running + partial_value.astype(jnp.float32)
    query_grad = lax.fori_loop(0, N_COL, query_step, jnp.zeros((QUERIES, D), jnp.float32))
    group_rows = Q_DEV * N_COL

    def doc_step(index, running):
        part_query = lax.dynamic_slice_in_dim(queries, index * group_rows, group_rows, 0)
        partial_value = jnp.zeros((DOCS, D), jnp.float32)
        for level_index in range(LEVELS):
            narrow = D >> level_index
            part_grad = lax.dynamic_slice_in_dim(grads[level_index], index * group_rows, group_rows, 0)
            contrib = lax.dot_general(part_grad, part_query[:, :narrow], (((0,), (0,)), ((), ())), preferred_element_type=jnp.float32) * math.sqrt(D / narrow)
            partial_value = partial_value + jnp.pad(contrib, ((0, 0), (0, D - narrow)))
        partial_value = partial_value.astype(jnp.bfloat16)
        partial_value = lax.optimization_barrier(partial_value)
        return running + partial_value.astype(jnp.float32)
    document_grad = lax.fori_loop(0, N_ROW, doc_step, jnp.zeros((DOCS, D), jnp.float32))
    return (mean_loss, query_grad.astype(jnp.bfloat16), document_grad.astype(jnp.bfloat16))
```

```python
import functools
import math

import jax
import jax.numpy as jnp
from jax import lax
from jax.experimental import pallas as pl
from jax.experimental.pallas import tpu as pltpu
from jax.sharding import PartitionSpec as P

MESH = pl.DeviceIdType.MESH
LEVELS = 4
X, YL, YH, Z = 4, 4, 2, 8
Y = YL * YH
QD, DD = 4, 8
CHUNKS = 2
NEAR = (1, 7, 2, 6, 3, 5, 4)
BF, F32 = jnp.bfloat16, jnp.float32


def wide(value):
    return value.astype(F32)


def kernel(
    q_ref, d_ref, p_ref, loss_ref, dq_ref, dd_ref,
    qbuf, pbuf, dbuf, qdense, pq, pd, sy, sx,
    xr1, xs2, xr2, yp, yr, ys, dsib, zp, zr, zs, lz, lk, dqv, ddv, sems, local,
):
    width = q_ref.shape[1]
    half, quarter = width // 2, width // (2 * CHUNKS)
    row = lax.axis_index("row")
    col = lax.axis_index("col")
    x = row // YL
    y = (col // (Z * 2)) * YL + row % YL
    z = (col // 2) % Z
    k = col % 2

    def at(ax, ay, az, ak):
        return (ax * YL + ay % YL, (ay // YL) * (Z * 2) + az * 2 + ak)

    def yo(o):
        return at(x, (y + o) % Y, z, k)

    def xo(o):
        return at((x + o) % X, y, z, k)

    def zo(o):
        return at(x, y, (z + o) % Z, k)

    sib = at(x, y, z, 1 - k)
    right, left, across = (x + 1) % X, (x + 3) % X, (x + 2) % X
    lo, hi = pl.ds(0, half), pl.ds(half, half)
    started = []

    def send(src, dst, dev):
        n = 2 * len(started)
        copy = pltpu.make_async_remote_copy(
            src_ref=src, dst_ref=dst, send_sem=sems.at[n], recv_sem=sems.at[n + 1],
            device_id=dev, device_id_type=MESH,
        )
        copy.start()
        started.append(copy)
        return copy

    load_q = pltpu.make_async_copy(q_ref, qbuf.at[x, y], local.at[0])
    load_d = pltpu.make_async_copy(d_ref, dbuf.at[k, z], local.at[1])
    load_q.start()
    load_d.start()
    barrier = pltpu.get_barrier_semaphore()
    peers = [zo(o) for o in NEAR] + [yo(o) for o in NEAR] + [xo(o) for o in (1, 3, 2)] + [sib]
    for dev in peers:
        pl.semaphore_signal(barrier, inc=1, device_id=dev, device_id_type=MESH)
    lanes = lax.broadcasted_iota(jnp.int32, (1, X * Y * QD), 1)
    spread = jnp.zeros_like(lanes)
    for i in range(QD):
        spread = jnp.where(lanes % QD == i, p_ref[i], spread)
    pbuf[x, y] = spread
    load_q.wait()
    load_d.wait()
    pl.semaphore_wait(barrier, len(peers))

    qy, qx, qh, dz, dk = {}, {}, {}, {}, {}

    def x_sends(o):
        block = qbuf.at[x, (y + Y - o) % Y]
        qx[o, 0] = send(block, block, xo(1))
        qx[o, 1] = send(block, block, xo(3))

    def x_relay(o):
        yy = (y + Y - o) % Y
        qx[o, 0].wait_recv()
        part = qbuf.at[left, yy, :, lo]
        qh[o, 0] = send(part, part, xo(1))
        qx[o, 1].wait_recv()
        part = qbuf.at[right, yy, :, hi]
        qh[o, 1] = send(part, part, xo(3))

    def y_take(o):
        if o == 4:
            qy[4, 0].wait_recv()
            qy[4, 1].wait_recv()
        else:
            qy[o].wait_recv()
        if o in (2, 6):
            yy = (y + Y - o) % Y
            block = qbuf.at[x, yy]
            near, far, piece = (1, 2, lo) if o == 2 else (7, 6, hi)
            qy[o + near - 8 * (o == 6)] = send(block, block, yo(near))
            part = qbuf.at[x, yy, :, piece]
            qy[4, int(o == 6)] = send(part, part, yo(far))
        x_sends(o)

    def z_take(o):
        if o == 4:
            dz[4, 0].wait_recv()
            dz[4, 1].wait_recv()
        else:
            dz[o].wait_recv()
        zz = (z + Z - o) % Z
        block = dbuf.at[k, zz]
        if o in (2, 6):
            near, far, piece = (1, 2, lo) if o == 2 else (7, 6, hi)
            dz[o + near - 8 * (o == 6)] = send(block, block, zo(near))
            part = dbuf.at[k, zz, :, piece]
            dz[4, int(o == 6)] = send(part, part, zo(far))
        dk[o] = send(block, block, sib)

    own = qbuf.at[x, y]
    for o in (2, 6, 1, 7):
        qy[o] = send(own, own, yo(o))
    x_sends(0)
    own = dbuf.at[k, z]
    for o in (2, 6, 1, 7):
        dz[o] = send(own, own, zo(o))
    pos_y = [send(pbuf.at[x, y], pbuf.at[x, y], yo(o)) for o in NEAR]
    dk[0] = send(own, own, sib)

    y_take(2)
    y_take(6)
    y_take(1)
    y_take(7)
    x_relay(0)
    z_take(2)
    z_take(6)
    y_take(3)
    y_take(5)
    y_take(4)
    x_relay(2)
    x_relay(6)
    z_take(1)
    z_take(7)
    x_relay(1)
    x_relay(7)
    for copy in pos_y:
        copy.wait_recv()
    pos_x = [send(pbuf.at[x], pbuf.at[x], xo(o)) for o in (1, 3, 2)]
    z_take(3)
    z_take(5)
    x_relay(3)
    x_relay(5)
    z_take(4)
    x_relay(4)
    for copy in pos_x:
        copy.wait_recv()
    for copy in dk.values():
        copy.wait_recv()
    for copy in qh.values():
        copy.wait_recv()

    step = min(512, width // 8)
    n_doc = 2 * Z * DD
    n_query = X * Y * QD
    for c in range(0, width, step):
        cs = pl.ds(c, step)
        for a in range(X):
            rows = [wide(qbuf[a, b, :, cs]) for b in range(Y)]
            qdense[a, :, cs] = jnp.concatenate(rows, axis=0).astype(BF)
    pos = jnp.zeros((1, n_query), jnp.int32)
    for a in range(X):
        for b in range(Y):
            pos = pos + jnp.where(lanes // QD == a * Y + b, pbuf[a, b], 0)
    subl = lax.broadcasted_iota(jnp.int32, (n_doc, n_query), 0)
    doc_id = (row * 2 * YH * Z + (col // (Z * 2)) * 2 * Z) * DD
    doc_id = doc_id + (subl // DD % Z) * 2 * DD + (subl // (DD * Z)) * DD + subl % DD
    onehot = jnp.where(doc_id == pos, 1.0, 0.0).astype(F32)

    edges = [0] + [width >> m for m in (3, 2, 1, 0)]
    logits = [None] * LEVELS
    running = None
    for s in range(LEVELS):
        first, end = edges[s], edges[s + 1]
        dpart = dbuf[:, :, :, first:end].reshape(n_doc, end - first)
        qpart = qdense[:, :, first:end].reshape(n_query, end - first)
        dots = lax.dot_general(
            dpart, qpart, (((1,), (1,)), ((), ())), preferred_element_type=F32
        )
        running = dots if running is None else running + dots
        logits[LEVELS - 1 - s] = running * (4.0 / math.sqrt(end))
    picked = jnp.zeros((1, n_query), F32)
    for m in range(LEVELS):
        largest = jnp.max(logits[m], axis=0, keepdims=True)
        sy[0, m : m + 1, :] = largest
        sy[0, LEVELS + m : LEVELS + m + 1, :] = jnp.sum(
            jnp.exp(logits[m] - largest), axis=0, keepdims=True
        )
        picked = picked + jnp.sum(onehot * logits[m], axis=0, keepdims=True)
    sy[0, 2 * LEVELS : 2 * LEVELS + 1, :] = picked

    def merged(ref, n):
        tops = [ref[i, 0:LEVELS, :] for i in range(n)]
        top = functools.reduce(jnp.maximum, tops)
        total = sum(ref[i, LEVELS : 2 * LEVELS, :] * jnp.exp(tops[i] - top) for i in range(n))
        return top, total, sum(ref[i, 2 * LEVELS : 2 * LEVELS + 1, :] for i in range(n))

    stats = [send(sy.at[0], sy.at[o], yo(o)) for o in NEAR]
    for copy in stats:
        copy.wait_recv()
    top, total, picked = merged(sy, Y)
    sx[0, 0:LEVELS, :] = top
    sx[0, LEVELS : 2 * LEVELS, :] = total
    sx[0, 2 * LEVELS : 2 * LEVELS + 1, :] = picked
    stats = [send(sx.at[0], sx.at[o], xo(o)) for o in (1, 3, 2)]
    for copy in stats:
        copy.wait_recv()
    top, total, picked = merged(sx, X)
    lse = top + jnp.log(total)

    grads = []
    weighted = None
    for m in range(LEVELS):
        grad = (jnp.exp(logits[m] - lse[m : m + 1, :]) - onehot) * math.sqrt(2.0**m)
        weighted = grad if weighted is None else weighted + grad
        grads.append(weighted)
    for s in range(LEVELS):
        first, end = edges[s], edges[s + 1]
        g = grads[LEVELS - 1 - s]
        gd = g.astype(BF)
        gq = g.T.astype(BF)
        for c in range(first, end, step):
            cs = pl.ds(c, step)
            part = jnp.dot(gd, qdense[:, :, cs].reshape(n_query, step), preferred_element_type=F32)
            pd[:, :, cs] = part.astype(BF).reshape(2, Z * DD, step)
            part = jnp.dot(gq, dbuf[:, :, :, cs].reshape(n_doc, step), preferred_element_type=F32)
            pq[:, :, cs] = part.astype(BF).reshape(X, Y * QD, step)

    def scatter_start(mine, into, dev):
        return {
            "a": send(mine(3), into(0), dev(1)),
            "A": send(mine(5), into(1), dev(7)),
            "b": send(mine(4, lo_of), into(2, lo_of), dev(2)),
            "B": send(mine(4, hi_of), into(2, hi_of), dev(6)),
            "c": send(mine(1), into(3), dev(1)),
            "C": send(mine(7), into(4), dev(7)),
        }

    def lo_of(n):
        return pl.ds(0, n // 2)

    def hi_of(n):
        return pl.ds(n // 2, n // 2)

    to_sib = send(pd.at[1 - k], dsib, sib)
    x_first, x_direct, x_relayed = {}, {}, {}

    def cols(side, c):
        return pl.ds(side * half + c * quarter, quarter)

    def x_start(c):
        x_first[c, 0] = send(pq.at[across, :, cols(0, c)], xr1.at[c, 0], xo(1))
        x_first[c, 1] = send(pq.at[across, :, cols(1, c)], xr1.at[c, 1], xo(3))

    def x_plain(c):
        x_direct[c, 0] = send(pq.at[right, :, cols(1, c)], xr2.at[c, 1], xo(1))
        x_direct[c, 1] = send(pq.at[left, :, cols(0, c)], xr2.at[c, 2], xo(3))

    def x_pass(c):
        for side, (via, slot, dev) in enumerate(((right, 0, xo(1)), (left, 3, xo(3)))):
            x_first[c, side].wait_recv()
            xs2[c, side] = (wide(pq[via, :, cols(side, c)]) + wide(xr1[c, side])).astype(BF)
            x_relayed[c, side] = send(xs2.at[c, side], xr2.at[c, slot], dev)

    def x_finish(c):
        for side in (0, 1):
            x_relayed[c, side].wait_recv()
            x_direct[c, side].wait_recv()
        for side in (0, 1):
            total = wide(pq[x, :, cols(side, c)]) + wide(xr2[c, side]) + wide(xr2[c, 2 + side])
            for b in range(Y):
                yp[c, b, :, side * quarter : (side + 1) * quarter] = total[
                    b * QD : (b + 1) * QD, :
                ].astype(BF)

    def y_start(c):
        def mine(o, part=None):
            ref = yp.at[c, (y + o) % Y]
            return ref if part is None else yp.at[c, (y + o) % Y, :, part(half)]

        def into(i, part=None):
            return yr.at[c, i] if part is None else yr.at[c, i, :, part(half)]

        return scatter_start(mine, into, yo)

    def y_pass(c, got):
        for side, names in enumerate(("ab", "AB")):
            for name in names:
                got[name].wait_recv()
            own = yp[c, (y + (2, 6)[side]) % Y]
            ys[c, side] = (wide(own) + wide(yr[c, side])).astype(BF)
            part = (lo_of, hi_of)[side](half)
            ys[c, side, :, part] = (
                wide(yp[c, (y + (2, 6)[side]) % Y, :, part])
                + wide(yr[c, side, :, part])
                + wide(yr[c, 2, :, part])
            ).astype(BF)
            got["dD"[side]] = send(ys.at[c, side], yr.at[c, 5 + side], yo((2, 6)[side]))

    for c in range(CHUNKS):
        x_start(c)
    x_plain(0)

    lz[0] = jnp.sum(lse, axis=0, keepdims=True) - picked
    losses = [send(lz.at[0], lz.at[o], zo(o)) for o in NEAR]

    to_sib.wait_recv()
    for b in range(Z):
        rows = slice(b * DD, (b + 1) * DD)
        zp[b] = (wide(pd[k, rows, :]) + wide(dsib[rows, :])).astype(BF)

    def z_mine(o, part=None):
        return zp.at[(z + o) % Z] if part is None else zp.at[(z + o) % Z, :, part(width)]

    def z_into(i, part=None):
        return zr.at[i] if part is None else zr.at[i, :, part(width)]

    zgot = scatter_start(z_mine, z_into, zo)
    x_pass(0)
    for c in range(1, CHUNKS):
        x_plain(c)
        x_pass(c)
    x_finish(0)
    ygot = {0: y_start(0)}
    for side, names in enumerate(("ab", "AB")):
        for name in names:
            zgot[name].wait_recv()
        zz = (z + (2, 6)[side]) % Z
        zs[side] = (wide(zp[zz]) + wide(zr[side])).astype(BF)
        part = (lo_of, hi_of)[side](width)
        zs[side, :, part] = (
            wide(zp[zz, :, part]) + wide(zr[side, :, part]) + wide(zr[2, :, part])
        ).astype(BF)
        zgot["dD"[side]] = send(zs.at[side], zr.at[5 + side], zo((2, 6)[side]))
    for c in range(1, CHUNKS):
        x_finish(c)
        ygot[c] = y_start(c)
    y_pass(0, ygot[0])
    for c in range(1, CHUNKS):
        y_pass(c, ygot[c])

    for copy in losses:
        copy.wait_recv()
    lk[0] = sum(lz[i] for i in range(Z))
    last = send(lk.at[0], lk.at[1], sib)
    for name in "cCdD":
        zgot[name].wait_recv()
    ddv[...] = (
        wide(zp[z]) + wide(zr[3]) + wide(zr[4]) + wide(zr[5]) + wide(zr[6])
    ).astype(BF)
    put_d = pltpu.make_async_copy(ddv, dd_ref, local.at[0])
    put_d.start()
    last.wait_recv()
    scale = 1.0 / (n_query * 2 * Z * LEVELS)
    loss_ref[...] = jnp.sum(lk[0] + lk[1], axis=1, keepdims=True) * scale
    for c in range(CHUNKS):
        for name in "cCdD":
            ygot[c][name].wait_recv()
        total = wide(yp[c, y]) + wide(yr[c, 3]) + wide(yr[c, 4]) + wide(yr[c, 5]) + wide(yr[c, 6])
        for side in (0, 1):
            dqv[:, cols(side, c)] = total[:, side * quarter : (side + 1) * quarter].astype(BF)
    put_q = pltpu.make_async_copy(dqv, dq_ref, local.at[1])
    put_q.start()
    for copy in started:
        copy.wait_send()
    put_d.wait()
    put_q.wait()


def shards(queries, documents, positive):
    width = queries.shape[1]
    half, quarter = width // 2, width // (2 * CHUNKS)
    n_query = X * Y * QD
    vm, dma = pltpu.VMEM, pltpu.SemaphoreType.DMA
    stat = 2 * LEVELS + 1
    anywhere = pl.BlockSpec(memory_space=pl.ANY)
    loss, dq, dd = pl.pallas_call(
        kernel,
        out_shape=[
            jax.ShapeDtypeStruct((1, 1), F32),
            jax.ShapeDtypeStruct(queries.shape, BF),
            jax.ShapeDtypeStruct(documents.shape, BF),
        ],
        in_specs=[anywhere, anywhere, pl.BlockSpec(memory_space=pltpu.SMEM)],
        out_specs=[pl.BlockSpec(memory_space=vm), anywhere, anywhere],
        scratch_shapes=[
            vm((X, Y, QD, width), BF),
            vm((X, Y, 1, n_query), jnp.int32),
            vm((2, Z, DD, width), BF),
            vm((X, Y * QD, width), BF),
            vm((X, Y * QD, width), BF),
            vm((2, Z * DD, width), BF),
            vm((Y, stat, n_query), F32),
            vm((X, stat, n_query), F32),
            vm((CHUNKS, 2, Y * QD, quarter), BF),
            vm((CHUNKS, 2, Y * QD, quarter), BF),
            vm((CHUNKS, 4, Y * QD, quarter), BF),
            vm((CHUNKS, Y, QD, half), BF),
            vm((CHUNKS, 7, QD, half), BF),
            vm((CHUNKS, 2, QD, half), BF),
            vm((Z * DD, width), BF),
            vm((Z, DD, width), BF),
            vm((7, DD, width), BF),
            vm((2, DD, width), BF),
            vm((Z, 1, n_query), F32),
            vm((2, 1, n_query), F32),
            vm(queries.shape, BF),
            vm(documents.shape, BF),
            dma((320,)),
            dma((2,)),
        ],
        compiler_params=pltpu.CompilerParams(collective_id=0, has_side_effects=True),
    )(queries, documents, positive)
    return (loss.reshape(()), dq, dd)


def solution(mesh):
    placed = (P(("row", "col"), None), P(("row", "col"), None), P(("row", "col")))
    return jax.shard_map(
        shards,
        mesh=mesh,
        in_specs=placed,
        out_specs=(P(), P(("row", "col"), None), P(("row", "col"), None)),
        check_vma=False,
    )
```

```python
import functools
import math

import jax
import jax.numpy as jnp
from jax import lax
from jax.experimental import pallas as pl
from jax.experimental.pallas import tpu as pltpu
from jax.sharding import PartitionSpec as P

MESH = pl.DeviceIdType.MESH
LEVELS = 4
X, YL, YH, Z = 4, 4, 2, 8
Y = YL * YH
QD, DD = 4, 8
CHUNKS = 2
ALT = 4
NEAR = (1, 7, 2, 6, 3, 5, 4)
BF, F32 = jnp.bfloat16, jnp.float32


def wide(value):
    return value.astype(F32)


def kernel(
    q_ref, d_ref, p_ref, loss_ref, dq_ref, dd_ref,
    qbuf, qalt, pbuf, dbuf, qdense, pq, pqa, pd, sy, sx,
    xr1, xs2, xr2, yp, yr, ys, ayr, ays, axp, axr, dsib, zp, zr, zs, lz, lk,
    lossv, dqv, ddv, psm, bulk, sems, out_sem, local,
):
    width = q_ref.shape[1]
    tail = width // ALT
    main = width - tail
    half, quarter = main // 2, main // (2 * CHUNKS)
    row = lax.axis_index("row")
    col = lax.axis_index("col")
    x = row // YL
    y = (col // (Z * 2)) * YL + row % YL
    z = (col // 2) % Z
    k = col % 2

    def at(ax, ay, az, ak):
        return (ax * YL + ay % YL, (ay // YL) * (Z * 2) + az * 2 + ak)

    def yo(o):
        return at(x, (y + o) % Y, z, k)

    def xo(o):
        return at((x + o) % X, y, z, k)

    def zo(o):
        return at(x, y, (z + o) % Z, k)

    sib = at(x, y, z, 1 - k)
    right, left, across = (x + 1) % X, (x + 3) % X, (x + 2) % X

    def lo_of(n):
        return pl.ds(0, n // 2)

    def hi_of(n):
        return pl.ds(n // 2, n // 2)

    slots = {}
    moved = []

    def sem_of(name):
        return sems.at[slots.setdefault(name, len(slots))]

    def send(src, dst, dev, name):
        moved.append(math.prod(src.shape) * (2 if src.dtype == BF else 4))
        pltpu.make_async_remote_copy(
            src_ref=src, dst_ref=dst, send_sem=out_sem, recv_sem=sem_of(name),
            device_id=dev, device_id_type=MESH,
        ).start()

    def take(name, ref):
        pltpu.make_async_copy(ref, ref, sem_of(name)).wait()

    def spread_start(own, dev, tag):
        for o in (2, 6, 1, 7):
            send(own, own, dev(o), (tag, o))

    def spread_take(o, block, part, dev, tag, n):
        if o == 4:
            take((tag, 4, 0), part(lo_of(n)))
            take((tag, 4, 1), part(hi_of(n)))
        else:
            take((tag, o), block)
        if o == 2:
            send(block, block, dev(1), (tag, 3))
            send(part(lo_of(n)), part(lo_of(n)), dev(2), (tag, 4, 0))
        if o == 6:
            send(block, block, dev(7), (tag, 5))
            send(part(hi_of(n)), part(hi_of(n)), dev(6), (tag, 4, 1))

    def scatter_start(mine, into, dev, tag):
        send(mine(3), into(0), dev(1), (tag, "a"))
        send(mine(5), into(1), dev(7), (tag, "A"))
        send(mine(4, lo_of), into(2, lo_of), dev(2), (tag, "b"))
        send(mine(4, hi_of), into(2, hi_of), dev(6), (tag, "B"))
        send(mine(1), into(3), dev(1), (tag, "c"))
        send(mine(7), into(4), dev(7), (tag, "c"))

    def scatter_pass(mine, into, through, dev, tag):
        for side, part in enumerate((lo_of, hi_of)):
            take((tag, "aA"[side]), into(side))
            take((tag, "bB"[side]), into(2, part))
            via = mine((2, 6)[side])
            out = through(side)
            out[...] = (wide(via[...]) + wide(into(side)[...])).astype(BF)
            piece = through(side, part)
            piece[...] = (
                wide(mine((2, 6)[side], part)[...])
                + wide(into(side, part)[...])
                + wide(into(2, part)[...])
            ).astype(BF)
            send(out, into(5 + side), dev((2, 6)[side]), (tag, "c"))

    loads = [
        pltpu.make_async_copy(q_ref.at[:, pl.ds(0, main)], qbuf.at[x, y], local.at[0]),
        pltpu.make_async_copy(q_ref.at[:, pl.ds(main, tail)], qalt.at[y, x], local.at[1]),
        pltpu.make_async_copy(d_ref, dbuf.at[k, z], local.at[2]),
    ]
    for copy in loads:
        copy.start()
    barrier = pltpu.get_barrier_semaphore()
    peers = [zo(o) for o in NEAR] + [yo(o) for o in NEAR] + [xo(o) for o in (1, 3, 2)] + [sib]
    for dev in peers:
        pl.semaphore_signal(barrier, inc=1, device_id=dev, device_id_type=MESH)
    lanes = lax.broadcasted_iota(jnp.int32, (1, X * Y * QD), 1)
    spread = jnp.zeros_like(lanes)
    for i in range(QD):
        spread = jnp.where(lanes % QD == i, p_ref[i], spread)
    pbuf[x, y] = spread
    for copy in loads:
        copy.wait()
    pl.semaphore_wait(barrier, len(peers))

    def qy_part(yy):
        return lambda cols=None: qbuf.at[x, yy] if cols is None else qbuf.at[x, yy, :, cols]

    def qa_part(yy):
        return lambda cols=None: qalt.at[yy] if cols is None else qalt.at[yy, :, :, cols]

    def dz_part(zz):
        return lambda cols=None: dbuf.at[k, zz] if cols is None else dbuf.at[k, zz, :, cols]

    def x_sends(o):
        block = qbuf.at[x, (y + Y - o) % Y]
        send(block, block, xo(1), ("qx", o, 0))
        send(block, block, xo(3), ("qx", o, 1))

    def x_relay(o):
        yy = (y + Y - o) % Y
        take(("qx", o, 0), qbuf.at[left, yy])
        part = qbuf.at[left, yy, :, lo_of(main)]
        send(part, part, xo(1), "qh")
        take(("qx", o, 1), qbuf.at[right, yy])
        part = qbuf.at[right, yy, :, hi_of(main)]
        send(part, part, xo(3), "qh")

    def y_take(o):
        yy = (y + Y - o) % Y
        spread_take(o, qbuf.at[x, yy], qy_part(yy), yo, "qy", main)
        x_sends(o)

    def a_take(o):
        yy = (y + Y - o) % Y
        spread_take(o, qalt.at[yy], qa_part(yy), yo, "qa", tail)

    def z_take(o):
        zz = (z + Z - o) % Z
        spread_take(o, dbuf.at[k, zz], dz_part(zz), zo, "dz", width)
        send(dbuf.at[k, zz], dbuf.at[k, zz], sib, "dk")

    spread_start(qbuf.at[x, y], yo, "qy")
    for o in (2, 1, 3):
        send(qalt.at[y, x], qalt.at[y, x], xo(o), "qax")
    x_sends(0)
    spread_start(dbuf.at[k, z], zo, "dz")
    for o in NEAR:
        send(pbuf.at[x, y], pbuf.at[x, y], yo(o), "py")
    send(dbuf.at[k, z], dbuf.at[k, z], sib, "dk")

    take("qax", qalt.at[0, pl.ds(0, X - 1)])
    spread_start(qalt.at[y], yo, "qa")
    y_take(2)
    y_take(6)
    y_take(1)
    y_take(7)
    x_relay(0)
    z_take(2)
    z_take(6)
    y_take(3)
    y_take(5)
    a_take(2)
    a_take(6)
    y_take(4)
    x_relay(2)
    x_relay(6)
    take("py", pbuf.at[0, pl.ds(0, Y - 1)])
    for o in (1, 3, 2):
        send(pbuf.at[x], pbuf.at[x], xo(o), "px")
    x_relay(1)
    x_relay(7)
    z_take(1)
    z_take(7)
    x_relay(3)
    x_relay(5)
    z_take(3)
    z_take(5)
    x_relay(4)
    z_take(4)
    for o in (1, 7, 3, 5, 4):
        a_take(o)
    take("px", pbuf.at[pl.ds(0, X - 1)])
    take("qh", qbuf.at[0])
    take("dk", dbuf.at[0])

    step = min(512, width // 8)
    n_doc = 2 * Z * DD
    n_query = X * Y * QD
    for c in range(0, width, step):
        cs = pl.ds(c, step)
        for a in range(X):
            if c < main:
                rows = [wide(qbuf[a, b, :, cs]) for b in range(Y)]
            else:
                rows = [wide(qalt[b, a, :, pl.ds(c - main, step)]) for b in range(Y)]
            qdense[a, :, cs] = jnp.concatenate(rows, axis=0).astype(BF)
    pos = jnp.zeros((1, n_query), jnp.int32)
    for a in range(X):
        for b in range(Y):
            pos = pos + jnp.where(lanes // QD == a * Y + b, pbuf[a, b], 0)
    subl = lax.broadcasted_iota(jnp.int32, (n_doc, n_query), 0)
    doc_id = (row * 2 * YH * Z + (col // (Z * 2)) * 2 * Z) * DD
    doc_id = doc_id + (subl // DD % Z) * 2 * DD + (subl // (DD * Z)) * DD + subl % DD
    onehot = jnp.where(doc_id == pos, 1.0, 0.0).astype(F32)

    edges = [0] + [width >> m for m in (3, 2, 1, 0)]
    logits = [None] * LEVELS
    running = None
    for s in range(LEVELS):
        first, end = edges[s], edges[s + 1]
        dpart = dbuf[:, :, :, first:end].reshape(n_doc, end - first)
        qpart = qdense[:, :, first:end].reshape(n_query, end - first)
        dots = lax.dot_general(
            dpart, qpart, (((1,), (1,)), ((), ())), preferred_element_type=F32
        )
        running = dots if running is None else running + dots
        logits[LEVELS - 1 - s] = running * (4.0 / math.sqrt(end))
    picked = jnp.zeros((1, n_query), F32)
    for m in range(LEVELS):
        largest = jnp.max(logits[m], axis=0, keepdims=True)
        sy[0, m : m + 1, :] = largest
        sy[0, LEVELS + m : LEVELS + m + 1, :] = jnp.sum(
            jnp.exp(logits[m] - largest), axis=0, keepdims=True
        )
        picked = picked + jnp.sum(onehot * logits[m], axis=0, keepdims=True)
    sy[0, 2 * LEVELS : 2 * LEVELS + 1, :] = picked

    def merged(ref, n):
        tops = [ref[i, 0:LEVELS, :] for i in range(n)]
        top = functools.reduce(jnp.maximum, tops)
        total = sum(ref[i, LEVELS : 2 * LEVELS, :] * jnp.exp(tops[i] - top) for i in range(n))
        return top, total, sum(ref[i, 2 * LEVELS : 2 * LEVELS + 1, :] for i in range(n))

    for o in (4, 3, 5, 2, 6, 1, 7):
        send(sy.at[0], sy.at[o], yo(o), "sy")
    take("sy", sy.at[pl.ds(1, Y - 1)])
    top, total, picked = merged(sy, Y)
    sx[0, 0:LEVELS, :] = top
    sx[0, LEVELS : 2 * LEVELS, :] = total
    sx[0, 2 * LEVELS : 2 * LEVELS + 1, :] = picked
    for o in (2, 1, 3):
        send(sx.at[0], sx.at[o], xo(o), "sx")
    take("sx", sx.at[pl.ds(1, X - 1)])
    top, total, picked = merged(sx, X)
    lse = top + jnp.log(total)

    grads = []
    weighted = None
    for m in range(LEVELS):
        grad = (jnp.exp(logits[m] - lse[m : m + 1, :]) - onehot) * math.sqrt(2.0**m)
        weighted = grad if weighted is None else weighted + grad
        grads.append(weighted)
    for s in range(LEVELS):
        first, end = edges[s], edges[s + 1]
        g = grads[LEVELS - 1 - s]
        gd = g.astype(BF)
        gq = g.T.astype(BF)
        for c in range(first, end, step):
            cs = pl.ds(c, step)
            part = jnp.dot(gd, qdense[:, :, cs].reshape(n_query, step), preferred_element_type=F32)
            pd[:, :, cs] = part.astype(BF).reshape(2, Z * DD, step)
            part = jnp.dot(gq, dbuf[:, :, :, cs].reshape(n_doc, step), preferred_element_type=F32)
            if c < main:
                pq[:, :, cs] = part.astype(BF).reshape(X, Y * QD, step)
            else:
                for a in range(X):
                    for b in range(Y):
                        at_row = (a * Y + b) * QD
                        pqa[b, a, :, pl.ds(c - main, step)] = part[at_row : at_row + QD, :].astype(BF)

    def cols(side, c):
        return pl.ds(side * half + c * quarter, quarter)

    def a_mine(o, part=None):
        yy = (y + o) % Y
        return pqa.at[yy] if part is None else pqa.at[yy, :, :, part(tail)]

    def a_into(i, part=None):
        return ayr.at[i] if part is None else ayr.at[i, :, :, part(tail)]

    def a_through(i, part=None):
        return ays.at[i] if part is None else ays.at[i, :, :, part(tail)]

    def x_start(c):
        send(pq.at[across, :, cols(0, c)], xr1.at[c, 0], xo(1), ("xa", c, 0))
        send(pq.at[across, :, cols(1, c)], xr1.at[c, 1], xo(3), ("xa", c, 1))

    def x_plain(c):
        send(pq.at[right, :, cols(1, c)], xr2.at[c, 1], xo(1), ("xc", c))
        send(pq.at[left, :, cols(0, c)], xr2.at[c, 2], xo(3), ("xc", c))

    def x_pass(c):
        for side, (via, slot, dev) in enumerate(((right, 0, xo(1)), (left, 3, xo(3)))):
            take(("xa", c, side), xr1.at[c, side])
            xs2[c, side] = (wide(pq[via, :, cols(side, c)]) + wide(xr1[c, side])).astype(BF)
            send(xs2.at[c, side], xr2.at[c, slot], dev, ("xc", c))

    def y_refs(c):
        def mine(o, part=None):
            yy = (y + o) % Y
            return yp.at[c, yy] if part is None else yp.at[c, yy, :, part(half)]

        def into(i, part=None):
            return yr.at[c, i] if part is None else yr.at[c, i, :, part(half)]

        def through(i, part=None):
            return ys.at[c, i] if part is None else ys.at[c, i, :, part(half)]

        return mine, into, through

    def x_finish(c):
        take(("xc", c), xr2.at[c])
        for side in (0, 1):
            total = wide(pq[x, :, cols(side, c)]) + wide(xr2[c, side]) + wide(xr2[c, 2 + side])
            for b in range(Y):
                yp[c, b, :, side * quarter : (side + 1) * quarter] = total[
                    b * QD : (b + 1) * QD, :
                ].astype(BF)
        mine, into, _ = y_refs(c)
        scatter_start(mine, into, yo, ("y", c))

    for c in range(CHUNKS):
        x_start(c)
    scatter_start(a_mine, a_into, yo, "ay")
    send(pd.at[1 - k], dsib, sib, "sib")
    x_plain(0)

    lz[0] = jnp.sum(lse, axis=0, keepdims=True) - picked
    for o in NEAR:
        send(lz.at[0], lz.at[o], zo(o), "lz")

    take("sib", dsib)
    for b in range(Z):
        rows = slice(b * DD, (b + 1) * DD)
        zp[b] = (wide(pd[k, rows, :]) + wide(dsib[rows, :])).astype(BF)

    def z_mine(o, part=None):
        zz = (z + o) % Z
        return zp.at[zz] if part is None else zp.at[zz, :, part(width)]

    def z_into(i, part=None):
        return zr.at[i] if part is None else zr.at[i, :, part(width)]

    def z_through(i, part=None):
        return zs.at[i] if part is None else zs.at[i, :, part(width)]

    scatter_start(z_mine, z_into, zo, "z")
    x_pass(0)
    for c in range(1, CHUNKS):
        x_plain(c)
        x_pass(c)
    scatter_pass(a_mine, a_into, a_through, yo, "ay")
    x_finish(0)
    scatter_pass(z_mine, z_into, z_through, zo, "z")
    take(("ay", "c"), ayr.at[pl.ds(3, 4)])
    for a in range(X):
        total = wide(pqa[y, a])
        for i in (3, 4, 5, 6):
            total = total + wide(ayr[i, a])
        axp[a] = total.astype(BF)
    for o in (2, 1, 3):
        send(axp.at[(x + o) % X], axr.at[o], xo(o), "ax")
    for c in range(1, CHUNKS):
        x_finish(c)
    take("lz", lz.at[pl.ds(1, Z - 1)])
    lk[0] = sum(lz[i] for i in range(Z))
    send(lk.at[0], lk.at[1], sib, "lk")
    for c in range(CHUNKS):
        scatter_pass(*y_refs(c), yo, ("y", c))
    take("ax", axr.at[pl.ds(1, X - 1)])
    total = wide(axp[x])
    for o in (1, 2, 3):
        total = total + wide(axr[o])
    dqv[:, main:] = total.astype(BF)
    take("lk", lk.at[1])
    scale = 1.0 / (n_query * 2 * Z * LEVELS)
    total = jnp.sum(lk[0] + lk[1], axis=1, keepdims=True) * scale
    lossv[...] = jnp.broadcast_to(total, (1, n_query))
    puts = [pltpu.make_async_copy(lossv, loss_ref, local.at[0])]
    puts[0].start()
    take(("z", "c"), zr.at[pl.ds(3, 4)])
    ddv[...] = (
        wide(zp[z]) + wide(zr[3]) + wide(zr[4]) + wide(zr[5]) + wide(zr[6])
    ).astype(BF)
    puts.append(pltpu.make_async_copy(ddv, dd_ref, local.at[1]))
    puts[1].start()
    for c in range(CHUNKS):
        take((("y", c), "c"), yr.at[c, pl.ds(3, 4)])
        total = wide(yp[c, y]) + wide(yr[c, 3]) + wide(yr[c, 4]) + wide(yr[c, 5]) + wide(yr[c, 6])
        for side in (0, 1):
            dqv[:, cols(side, c)] = total[:, side * quarter : (side + 1) * quarter].astype(BF)
    puts.append(pltpu.make_async_copy(dqv, dq_ref, local.at[2]))
    puts[2].start()
    sent = bulk.at[pl.ds(0, sum(moved) // 512)]
    pltpu.make_async_copy(sent, sent, out_sem).wait()
    for copy in puts:
        copy.wait()


def shards(queries, documents, positive):
    width = queries.shape[1]
    tail = width // ALT
    main = width - tail
    half, quarter = main // 2, main // (2 * CHUNKS)
    n_query = X * Y * QD
    vm, dma = pltpu.VMEM, pltpu.SemaphoreType.DMA
    stat = 2 * LEVELS + 1
    anywhere = pl.BlockSpec(memory_space=pl.ANY)
    loss, dq, dd = pl.pallas_call(
        kernel,
        out_shape=[
            jax.ShapeDtypeStruct((1, n_query), F32),
            jax.ShapeDtypeStruct(queries.shape, BF),
            jax.ShapeDtypeStruct(documents.shape, BF),
        ],
        in_specs=[anywhere, anywhere, pl.BlockSpec(memory_space=pltpu.SMEM)],
        out_specs=[anywhere] * 3,
        scratch_shapes=[
            vm((X, Y, QD, main), BF),
            vm((Y, X, QD, tail), BF),
            vm((X, Y, 1, n_query), jnp.int32),
            vm((2, Z, DD, width), BF),
            vm((X, Y * QD, width), BF),
            vm((X, Y * QD, main), BF),
            vm((Y, X, QD, tail), BF),
            vm((2, Z * DD, width), BF),
            vm((Y, stat, n_query), F32),
            vm((X, stat, n_query), F32),
            vm((CHUNKS, 2, Y * QD, quarter), BF),
            vm((CHUNKS, 2, Y * QD, quarter), BF),
            vm((CHUNKS, 4, Y * QD, quarter), BF),
            vm((CHUNKS, Y, QD, half), BF),
            vm((CHUNKS, 7, QD, half), BF),
            vm((CHUNKS, 2, QD, half), BF),
            vm((7, X, QD, tail), BF),
            vm((2, X, QD, tail), BF),
            vm((X, QD, tail), BF),
            vm((X, QD, tail), BF),
            vm((Z * DD, width), BF),
            vm((Z, DD, width), BF),
            vm((7, DD, width), BF),
            vm((2, DD, width), BF),
            vm((Z, 1, n_query), F32),
            vm((2, 1, n_query), F32),
            vm((1, n_query), F32),
            vm(queries.shape, BF),
            vm(documents.shape, BF),
            pltpu.SMEM((QD,), jnp.int32),
            vm((16384, 128), F32),
            dma((80,)),
            dma,
            dma((3,)),
        ],
        compiler_params=pltpu.CompilerParams(collective_id=0, has_side_effects=True),
    )(queries, documents, positive)
    return (loss[0, 0], dq, dd)


def solution(mesh):
    placed = (P(("row", "col"), None), P(("row", "col"), None), P(("row", "col")))
    return jax.shard_map(
        shards,
        mesh=mesh,
        in_specs=placed,
        out_specs=(P(), P(("row", "col"), None), P(("row", "col"), None)),
        check_vma=False,
    )
```

```python
import functools
import math

import jax
import jax.numpy as jnp
from jax import lax
from jax.experimental import pallas as pl
from jax.experimental.pallas import tpu as pltpu
from jax.sharding import PartitionSpec as P

MESH = pl.DeviceIdType.MESH
LEVELS = 4
X, YL, YH, Z = 4, 4, 2, 8
Y = YL * YH
QD, DD = 4, 8
ALT = 5 / 16
FAR = (4, 3, 5, 2, 6, 1, 7)
NEAR = (1, 7, 2, 6, 3, 5, 4)
BF, F32 = jnp.bfloat16, jnp.float32


def wide(value):
    return value.astype(F32)


def kernel(
    q_ref, d_ref, p_ref, loss_ref, dq_ref, dd_ref,
    qbuf, qalt, pbuf, dbuf, qdense, pq, pqa, pd, sy, sx,
    xr, yp, yr, ayr, ays, axp, axr, dsib, zp, zr, zs, lz, lk,
    lossv, dqv, ddv, bulk, sems, out_sem, local,
):
    width = q_ref.shape[1]
    tail = int(width * ALT)
    main = width - tail
    row = lax.axis_index("row")
    col = lax.axis_index("col")
    x = row // YL
    y = (col // (Z * 2)) * YL + row % YL
    z = (col // 2) % Z
    k = col % 2

    def at(ax, ay, az, ak):
        return (ax * YL + ay % YL, (ay // YL) * (Z * 2) + az * 2 + ak)

    def yo(o):
        return at(x, (y + o) % Y, z, k)

    def xo(o):
        return at((x + o) % X, y, z, k)

    def zo(o):
        return at(x, y, (z + o) % Z, k)

    sib = at(x, y, z, 1 - k)

    def lo_of(n):
        return pl.ds(0, n // 2)

    def hi_of(n):
        return pl.ds(n // 2, n // 2)

    slots = {}
    moved = []

    def sem_of(name):
        return sems.at[slots.setdefault(name, len(slots))]

    def send(src, dst, dev, name):
        moved.append(math.prod(src.shape) * (2 if src.dtype == BF else 4))
        pltpu.make_async_remote_copy(
            src_ref=src, dst_ref=dst, send_sem=out_sem, recv_sem=sem_of(name),
            device_id=dev, device_id_type=MESH,
        ).start()

    def take(name, ref):
        pltpu.make_async_copy(ref, ref, sem_of(name)).wait()

    def spread_start(own, dev, tag):
        for o in (2, 6, 1, 7):
            send(own, own, dev(o), (tag, o))

    def spread_take(o, block, part, dev, tag, n):
        if o == 4:
            take((tag, 4, 0), part(lo_of(n)))
            take((tag, 4, 1), part(hi_of(n)))
        else:
            take((tag, o), block)
        if o == 2:
            send(block, block, dev(1), (tag, 3))
            send(part(lo_of(n)), part(lo_of(n)), dev(2), (tag, 4, 0))
        if o == 6:
            send(block, block, dev(7), (tag, 5))
            send(part(hi_of(n)), part(hi_of(n)), dev(6), (tag, 4, 1))

    def scatter_start(mine, into, dev, tag):
        send(mine(3), into(0), dev(1), (tag, "a"))
        send(mine(5), into(1), dev(7), (tag, "A"))
        send(mine(4, lo_of), into(2, lo_of), dev(2), (tag, "b"))
        send(mine(4, hi_of), into(2, hi_of), dev(6), (tag, "B"))
        send(mine(1), into(3), dev(1), (tag, "c"))
        send(mine(7), into(4), dev(7), (tag, "c"))

    def scatter_pass(mine, into, through, dev, tag):
        for side, part in enumerate((lo_of, hi_of)):
            take((tag, "aA"[side]), into(side))
            take((tag, "bB"[side]), into(2, part))
            via = mine((2, 6)[side])
            out = through(side)
            out[...] = (wide(via[...]) + wide(into(side)[...])).astype(BF)
            piece = through(side, part)
            piece[...] = (
                wide(mine((2, 6)[side], part)[...])
                + wide(into(side, part)[...])
                + wide(into(2, part)[...])
            ).astype(BF)
            send(out, into(5 + side), dev((2, 6)[side]), (tag, "c"))

    loads = [
        pltpu.make_async_copy(q_ref.at[:, pl.ds(0, main)], qbuf.at[x, y], local.at[0]),
        pltpu.make_async_copy(q_ref.at[:, pl.ds(main, tail)], qalt.at[y, x], local.at[1]),
        pltpu.make_async_copy(d_ref, dbuf.at[k, z], local.at[2]),
    ]
    for copy in loads:
        copy.start()
    barrier = pltpu.get_barrier_semaphore()
    peers = [zo(o) for o in NEAR] + [yo(o) for o in NEAR] + [xo(o) for o in (1, 3, 2)] + [sib]
    for dev in peers:
        pl.semaphore_signal(barrier, inc=1, device_id=dev, device_id_type=MESH)
    lanes = lax.broadcasted_iota(jnp.int32, (1, X * Y * QD), 1)
    spread = jnp.zeros_like(lanes)
    for i in range(QD):
        spread = jnp.where(lanes % QD == i, p_ref[i], spread)
    pbuf[x, y] = spread
    for copy in loads:
        copy.wait()
    pl.semaphore_wait(barrier, len(peers))

    def qa_part(yy):
        return lambda cols=None: qalt.at[yy] if cols is None else qalt.at[yy, :, :, cols]

    def dz_part(zz):
        return lambda cols=None: dbuf.at[k, zz] if cols is None else dbuf.at[k, zz, :, cols]

    def x_sends(o):
        block = qbuf.at[x, (y + Y - o) % Y]
        for dx in (2, 1, 3):
            send(block, block, xo(dx), "qx")

    def y_take(o):
        take(("qy", o), qbuf.at[x, y])
        x_sends(o)

    def a_take(o):
        yy = (y + Y - o) % Y
        spread_take(o, qalt.at[yy], qa_part(yy), yo, "qa", tail)

    def z_take(o):
        zz = (z + Z - o) % Z
        spread_take(o, dbuf.at[k, zz], dz_part(zz), zo, "dz", width)
        send(dbuf.at[k, zz], dbuf.at[k, zz], sib, "dk")

    for o in NEAR:
        send(qbuf.at[x, y], qbuf.at[x, y], yo(o), ("qy", o))
    for o in (2, 1, 3):
        send(qalt.at[y, x], qalt.at[y, x], xo(o), "qax")
    x_sends(0)
    spread_start(dbuf.at[k, z], zo, "dz")
    for o in NEAR:
        send(pbuf.at[x, y], pbuf.at[x, y], yo(o), "py")
    send(dbuf.at[k, z], dbuf.at[k, z], sib, "dk")

    y_take(1)
    y_take(7)
    take("qax", qalt.at[0, pl.ds(0, X - 1)])
    spread_start(qalt.at[y], yo, "qa")
    y_take(2)
    y_take(6)
    z_take(2)
    z_take(6)
    y_take(3)
    y_take(5)
    y_take(4)
    a_take(2)
    a_take(6)
    take("py", pbuf.at[0, pl.ds(0, Y - 1)])
    for o in (1, 3, 2):
        send(pbuf.at[x], pbuf.at[x], xo(o), "px")
    for o in (1, 7, 3, 5, 4):
        z_take(o)
    for o in (1, 7, 3, 5, 4):
        a_take(o)
    take("px", pbuf.at[pl.ds(0, X - 1)])
    take("qx", qbuf.at[pl.ds(0, X - 1)])
    take("dk", dbuf.at[0])

    step = min(512, width // 8)
    n_doc = 2 * Z * DD
    n_query = X * Y * QD

    def pieces(first, end):
        cuts = sorted({*range(first, end, step), end} | ({main} if first < main < end else set()))
        return [(c, d - c) for c, d in zip(cuts, cuts[1:])]

    for c, n in pieces(0, width):
        cs = pl.ds(c, n)
        for a in range(X):
            if c < main:
                rows = [wide(qbuf[a, b, :, cs]) for b in range(Y)]
            else:
                rows = [wide(qalt[b, a, :, pl.ds(c - main, n)]) for b in range(Y)]
            qdense[a, :, cs] = jnp.concatenate(rows, axis=0).astype(BF)
    pos = jnp.zeros((1, n_query), jnp.int32)
    for a in range(X):
        for b in range(Y):
            pos = pos + jnp.where(lanes // QD == a * Y + b, pbuf[a, b], 0)
    subl = lax.broadcasted_iota(jnp.int32, (n_doc, n_query), 0)
    doc_id = (row * 2 * YH * Z + (col // (Z * 2)) * 2 * Z) * DD
    doc_id = doc_id + (subl // DD % Z) * 2 * DD + (subl // (DD * Z)) * DD + subl % DD
    onehot = jnp.where(doc_id == pos, 1.0, 0.0).astype(F32)

    edges = [0] + [width >> m for m in (3, 2, 1, 0)]
    logits = [None] * LEVELS
    running = None
    for s in range(LEVELS):
        first, end = edges[s], edges[s + 1]
        dpart = dbuf[:, :, :, first:end].reshape(n_doc, end - first)
        qpart = qdense[:, :, first:end].reshape(n_query, end - first)
        dots = lax.dot_general(
            dpart, qpart, (((1,), (1,)), ((), ())), preferred_element_type=F32
        )
        running = dots if running is None else running + dots
        logits[LEVELS - 1 - s] = running * (4.0 / math.sqrt(end))
    picked = jnp.zeros((1, n_query), F32)
    for m in range(LEVELS):
        largest = jnp.max(logits[m], axis=0, keepdims=True)
        sy[0, m : m + 1, :] = largest
        sy[0, LEVELS + m : LEVELS + m + 1, :] = jnp.sum(
            jnp.exp(logits[m] - largest), axis=0, keepdims=True
        )
        picked = picked + jnp.sum(onehot * logits[m], axis=0, keepdims=True)
    sy[0, 2 * LEVELS : 2 * LEVELS + 1, :] = picked

    def merged(ref, n):
        tops = [ref[i, 0:LEVELS, :] for i in range(n)]
        top = functools.reduce(jnp.maximum, tops)
        total = sum(ref[i, LEVELS : 2 * LEVELS, :] * jnp.exp(tops[i] - top) for i in range(n))
        return top, total, sum(ref[i, 2 * LEVELS : 2 * LEVELS + 1, :] for i in range(n))

    for o in (4, 3, 5, 2, 6, 1, 7):
        send(sy.at[0], sy.at[o], yo(o), "sy")
    take("sy", sy.at[pl.ds(1, Y - 1)])
    top, total, picked = merged(sy, Y)
    sx[0, 0:LEVELS, :] = top
    sx[0, LEVELS : 2 * LEVELS, :] = total
    sx[0, 2 * LEVELS : 2 * LEVELS + 1, :] = picked
    for o in (2, 1, 3):
        send(sx.at[0], sx.at[o], xo(o), "sx")
    take("sx", sx.at[pl.ds(1, X - 1)])
    top, total, picked = merged(sx, X)
    lse = top + jnp.log(total)

    grads = []
    weighted = None
    for m in range(LEVELS):
        grad = (jnp.exp(logits[m] - lse[m : m + 1, :]) - onehot) * math.sqrt(2.0**m)
        weighted = grad if weighted is None else weighted + grad
        grads.append(weighted)
    for s in range(LEVELS):
        first, end = edges[s], edges[s + 1]
        g = grads[LEVELS - 1 - s]
        gd = g.astype(BF)
        gq = g.T.astype(BF)
        for c, n in pieces(first, end):
            part = jnp.dot(gd, qdense[:, :, c : c + n].reshape(n_query, n), preferred_element_type=F32)
            pd[:, :, c : c + n] = part.astype(BF).reshape(2, Z * DD, n)
            part = jnp.dot(gq, dbuf[:, :, :, c : c + n].reshape(n_doc, n), preferred_element_type=F32)
            for a in range(X):
                for b in range(Y):
                    at_row = (a * Y + b) * QD
                    block = part[at_row : at_row + QD, :].astype(BF)
                    if c < main:
                        pq[a, b, :, c : c + n] = block
                    else:
                        pqa[b, a, :, c - main : c - main + n] = block

    def a_mine(o, part=None):
        yy = (y + o) % Y
        return pqa.at[yy] if part is None else pqa.at[yy, :, :, part(tail)]

    def a_into(i, part=None):
        return ayr.at[i] if part is None else ayr.at[i, :, :, part(tail)]

    def a_through(i, part=None):
        return ays.at[i] if part is None else ays.at[i, :, :, part(tail)]

    def x_start(o):
        yy = (y + o) % Y
        for dx in (2, 1, 3):
            send(pq.at[(x + dx) % X, yy], xr.at[o, dx - 1], xo(dx), ("x", o))

    def x_finish(o):
        take(("x", o), xr.at[o])
        total = wide(pq[x, (y + o) % Y])
        for i in range(X - 1):
            total = total + wide(xr[o, i])
        if o:
            yp[o] = total.astype(BF)
            send(yp.at[o], yr.at[o], yo(o), "y")
        return total

    x_start(4)
    scatter_start(a_mine, a_into, yo, "ay")
    send(pd.at[1 - k], dsib, sib, "sib")
    for o in FAR[1:] + (0,):
        x_start(o)

    lz[0] = jnp.sum(lse, axis=0, keepdims=True) - picked
    for o in NEAR:
        send(lz.at[0], lz.at[o], zo(o), "lz")

    take("sib", dsib)
    for b in range(Z):
        rows = slice(b * DD, (b + 1) * DD)
        zp[b] = (wide(pd[k, rows, :]) + wide(dsib[rows, :])).astype(BF)

    def z_mine(o, part=None):
        zz = (z + o) % Z
        return zp.at[zz] if part is None else zp.at[zz, :, part(width)]

    def z_into(i, part=None):
        return zr.at[i] if part is None else zr.at[i, :, part(width)]

    def z_through(i, part=None):
        return zs.at[i] if part is None else zs.at[i, :, part(width)]

    scatter_start(z_mine, z_into, zo, "z")
    x_finish(4)
    x_finish(3)
    x_finish(5)
    scatter_pass(a_mine, a_into, a_through, yo, "ay")
    x_finish(2)
    x_finish(6)
    scatter_pass(z_mine, z_into, z_through, zo, "z")
    take(("ay", "c"), ayr.at[pl.ds(3, 4)])
    for a in range(X):
        total = wide(pqa[y, a])
        for i in (3, 4, 5, 6):
            total = total + wide(ayr[i, a])
        axp[a] = total.astype(BF)
    for o in (2, 1, 3):
        send(axp.at[(x + o) % X], axr.at[o], xo(o), "ax")
    x_finish(1)
    x_finish(7)
    take("lz", lz.at[pl.ds(1, Z - 1)])
    lk[0] = sum(lz[i] for i in range(Z))
    send(lk.at[0], lk.at[1], sib, "lk")
    take("ax", axr.at[pl.ds(1, X - 1)])
    total = wide(axp[x])
    for o in (1, 2, 3):
        total = total + wide(axr[o])
    dqv[:, main:] = total.astype(BF)
    take("lk", lk.at[1])
    scale = 1.0 / (n_query * 2 * Z * LEVELS)
    total = jnp.sum(lk[0] + lk[1], axis=1, keepdims=True) * scale
    lossv[...] = jnp.broadcast_to(total, (1, n_query))
    puts = [pltpu.make_async_copy(lossv, loss_ref, local.at[0])]
    puts[0].start()
    take(("z", "c"), zr.at[pl.ds(3, 4)])
    ddv[...] = (
        wide(zp[z]) + wide(zr[3]) + wide(zr[4]) + wide(zr[5]) + wide(zr[6])
    ).astype(BF)
    puts.append(pltpu.make_async_copy(ddv, dd_ref, local.at[1]))
    puts[1].start()
    total = x_finish(0)
    take("y", yr.at[pl.ds(1, Y - 1)])
    for o in NEAR:
        total = total + wide(yr[o])
    dqv[:, :main] = total.astype(BF)
    puts.append(pltpu.make_async_copy(dqv, dq_ref, local.at[2]))
    puts[2].start()
    sent = bulk.at[pl.ds(0, sum(moved) // 512)]
    pltpu.make_async_copy(sent, sent, out_sem).wait()
    for copy in puts:
        copy.wait()


def shards(queries, documents, positive):
    width = queries.shape[1]
    tail = int(width * ALT)
    main = width - tail
    n_query = X * Y * QD
    vm, dma = pltpu.VMEM, pltpu.SemaphoreType.DMA
    stat = 2 * LEVELS + 1
    anywhere = pl.BlockSpec(memory_space=pl.ANY)
    loss, dq, dd = pl.pallas_call(
        kernel,
        out_shape=[
            jax.ShapeDtypeStruct((1, n_query), F32),
            jax.ShapeDtypeStruct(queries.shape, BF),
            jax.ShapeDtypeStruct(documents.shape, BF),
        ],
        in_specs=[anywhere, anywhere, pl.BlockSpec(memory_space=pltpu.SMEM)],
        out_specs=[anywhere] * 3,
        scratch_shapes=[
            vm((X, Y, QD, main), BF),
            vm((Y, X, QD, tail), BF),
            vm((X, Y, 1, n_query), jnp.int32),
            vm((2, Z, DD, width), BF),
            vm((X, Y * QD, width), BF),
            vm((X, Y, QD, main), BF),
            vm((Y, X, QD, tail), BF),
            vm((2, Z * DD, width), BF),
            vm((Y, stat, n_query), F32),
            vm((X, stat, n_query), F32),
            vm((Y, X - 1, QD, main), BF),
            vm((Y, QD, main), BF),
            vm((Y, QD, main), BF),
            vm((7, X, QD, tail), BF),
            vm((2, X, QD, tail), BF),
            vm((X, QD, tail), BF),
            vm((X, QD, tail), BF),
            vm((Z * DD, width), BF),
            vm((Z, DD, width), BF),
            vm((7, DD, width), BF),
            vm((2, DD, width), BF),
            vm((Z, 1, n_query), F32),
            vm((2, 1, n_query), F32),
            vm((1, n_query), F32),
            vm(queries.shape, BF),
            vm(documents.shape, BF),
            vm((16384, 128), F32),
            dma((54,)),
            dma,
            dma((3,)),
        ],
        compiler_params=pltpu.CompilerParams(collective_id=0, has_side_effects=True),
    )(queries, documents, positive)
    return (loss[0, 0], dq, dd)


def solution(mesh):
    placed = (P(("row", "col"), None), P(("row", "col"), None), P(("row", "col")))
    return jax.shard_map(
        shards,
        mesh=mesh,
        in_specs=placed,
        out_specs=(P(), P(("row", "col"), None), P(("row", "col"), None)),
        check_vma=False,
    )
```

```python
import functools
import math

import jax
import jax.numpy as jnp
from jax import lax
from jax.experimental import pallas as pl
from jax.experimental.pallas import tpu as pltpu
from jax.sharding import PartitionSpec as P

MESH = pl.DeviceIdType.MESH
LEVELS = 4
X, YL, YH, Z = 4, 4, 2, 8
Y = YL * YH
QD, DD = 4, 8
ALT = 5 / 16
FAR = (4, 3, 5, 2, 6, 1, 7)
NEAR = (1, 7, 2, 6, 3, 5, 4)
BF, F32 = jnp.bfloat16, jnp.float32


def wide(value):
    return value.astype(F32)


def kernel(
    q_ref, d_ref, p_ref, loss_ref, dq_ref, dd_ref,
    qbuf, qalt, pbuf, dbuf, qdense, pq, pqa, pd, sy, sx,
    xr, yp, yr, ayr, ays, axp, axr, dsib, zp, zr, zs, lz, lk,
    lossv, dqv, ddv, psm, bulk, sems, out_sem, local,
):
    width = q_ref.shape[1]
    tail = int(width * ALT)
    main = width - tail
    row = lax.axis_index("row")
    col = lax.axis_index("col")
    x = row // YL
    y = (col // (Z * 2)) * YL + row % YL
    z = (col // 2) % Z
    k = col % 2

    def at(ax, ay, az, ak):
        return (ax * YL + ay % YL, (ay // YL) * (Z * 2) + az * 2 + ak)

    def yo(o):
        return at(x, (y + o) % Y, z, k)

    def xo(o):
        return at((x + o) % X, y, z, k)

    def zo(o):
        return at(x, y, (z + o) % Z, k)

    sib = at(x, y, z, 1 - k)

    def lo_of(n):
        return pl.ds(0, n // 2)

    def hi_of(n):
        return pl.ds(n // 2, n // 2)

    slots = {}
    moved = []

    def sem_of(name):
        return sems.at[slots.setdefault(name, len(slots))]

    def send(src, dst, dev, name):
        moved.append(math.prod(src.shape) * (2 if src.dtype == BF else 4))
        pltpu.make_async_remote_copy(
            src_ref=src, dst_ref=dst, send_sem=out_sem, recv_sem=sem_of(name),
            device_id=dev, device_id_type=MESH,
        ).start()

    def take(name, ref):
        pltpu.make_async_copy(ref, ref, sem_of(name)).wait()

    def spread_start(own, dev, tag):
        for o in (2, 6, 1, 7):
            send(own, own, dev(o), (tag, o))

    def spread_take(o, block, part, dev, tag, n):
        if o == 4:
            take((tag, 4, 0), part(lo_of(n)))
            take((tag, 4, 1), part(hi_of(n)))
        else:
            take((tag, o), block)
        if o == 2:
            send(block, block, dev(1), (tag, 3))
            send(part(lo_of(n)), part(lo_of(n)), dev(2), (tag, 4, 0))
        if o == 6:
            send(block, block, dev(7), (tag, 5))
            send(part(hi_of(n)), part(hi_of(n)), dev(6), (tag, 4, 1))

    def scatter_start(mine, into, dev, tag):
        send(mine(3), into(0), dev(1), (tag, "a"))
        send(mine(5), into(1), dev(7), (tag, "A"))
        send(mine(4, lo_of), into(2, lo_of), dev(2), (tag, "b"))
        send(mine(4, hi_of), into(2, hi_of), dev(6), (tag, "B"))
        send(mine(1), into(3), dev(1), (tag, "c"))
        send(mine(7), into(4), dev(7), (tag, "c"))

    def scatter_pass(mine, into, through, dev, tag):
        for side, part in enumerate((lo_of, hi_of)):
            take((tag, "aA"[side]), into(side))
            take((tag, "bB"[side]), into(2, part))
            via = mine((2, 6)[side])
            out = through(side)
            out[...] = (wide(via[...]) + wide(into(side)[...])).astype(BF)
            piece = through(side, part)
            piece[...] = (
                wide(mine((2, 6)[side], part)[...])
                + wide(into(side, part)[...])
                + wide(into(2, part)[...])
            ).astype(BF)
            send(out, into(5 + side), dev((2, 6)[side]), (tag, "c"))

    load_p = pltpu.make_async_copy(p_ref, psm, local.at[3])
    load_p.start()
    loads = [
        pltpu.make_async_copy(q_ref.at[:, pl.ds(0, main)], qbuf.at[x, y], local.at[0]),
        pltpu.make_async_copy(q_ref.at[:, pl.ds(main, tail)], qalt.at[y, x], local.at[1]),
        pltpu.make_async_copy(d_ref, dbuf.at[k, z], local.at[2]),
    ]
    for copy in loads:
        copy.start()
    barrier = pltpu.get_barrier_semaphore()
    peers = [zo(o) for o in NEAR] + [yo(o) for o in NEAR] + [xo(o) for o in (1, 3, 2)] + [sib]
    for dev in peers:
        pl.semaphore_signal(barrier, inc=1, device_id=dev, device_id_type=MESH)
    lanes = lax.broadcasted_iota(jnp.int32, (1, X * Y * QD), 1)
    for copy in loads:
        copy.wait()
    pl.semaphore_wait(barrier, len(peers))

    def qa_part(yy):
        return lambda cols=None: qalt.at[yy] if cols is None else qalt.at[yy, :, :, cols]

    def dz_part(zz):
        return lambda cols=None: dbuf.at[k, zz] if cols is None else dbuf.at[k, zz, :, cols]

    def x_sends(o):
        block = qbuf.at[x, (y + Y - o) % Y]
        for dx in (2, 1, 3):
            send(block, block, xo(dx), "qx")

    def y_take(o):
        take(("qy", o), qbuf.at[x, y])
        x_sends(o)

    def a_take(o):
        yy = (y + Y - o) % Y
        spread_take(o, qalt.at[yy], qa_part(yy), yo, "qa", tail)

    def z_take(o):
        zz = (z + Z - o) % Z
        spread_take(o, dbuf.at[k, zz], dz_part(zz), zo, "dz", width)
        send(dbuf.at[k, zz], dbuf.at[k, zz], sib, "dk")

    for o in NEAR:
        send(qbuf.at[x, y], qbuf.at[x, y], yo(o), ("qy", o))
    for o in (2, 1, 3):
        send(qalt.at[y, x], qalt.at[y, x], xo(o), "qax")
    x_sends(0)
    spread_start(dbuf.at[k, z], zo, "dz")
    load_p.wait()
    spread = jnp.zeros_like(lanes)
    for i in range(QD):
        spread = jnp.where(lanes % QD == i, psm[i], spread)
    pbuf[x, y] = spread
    for o in NEAR:
        send(pbuf.at[x, y], pbuf.at[x, y], yo(o), "py")
    send(dbuf.at[k, z], dbuf.at[k, z], sib, "dk")

    y_take(1)
    y_take(7)
    take("qax", qalt.at[0, pl.ds(0, X - 1)])
    spread_start(qalt.at[y], yo, "qa")
    y_take(2)
    y_take(6)
    z_take(2)
    z_take(6)
    y_take(3)
    y_take(5)
    y_take(4)
    a_take(2)
    a_take(6)
    take("py", pbuf.at[0, pl.ds(0, Y - 1)])
    for o in (1, 3, 2):
        send(pbuf.at[x], pbuf.at[x], xo(o), "px")
    for o in (1, 7, 3, 5, 4):
        z_take(o)
    step = min(512, width // 8)
    n_doc = 2 * Z * DD
    n_query = X * Y * QD

    def pieces(first, end):
        cuts = sorted({*range(first, end, step), end} | ({main} if first < main < end else set()))
        return [(c, d - c) for c, d in zip(cuts, cuts[1:])]

    def densify(first, end, block):
        for c, n in pieces(first, end):
            for a in range(X):
                rows = [wide(block(a, b, c, n)) for b in range(Y)]
                qdense[a, :, c : c + n] = jnp.concatenate(rows, axis=0).astype(BF)

    take("qx", qbuf.at[pl.ds(0, X - 1)])
    densify(0, main, lambda a, b, c, n: qbuf[a, b, :, c : c + n])
    for o in (1, 7, 3, 5, 4):
        a_take(o)
    densify(main, width, lambda a, b, c, n: qalt[b, a, :, c - main : c - main + n])
    take("px", pbuf.at[pl.ds(0, X - 1)])
    take("dk", dbuf.at[0])
    pos = jnp.zeros((1, n_query), jnp.int32)
    for a in range(X):
        for b in range(Y):
            pos = pos + jnp.where(lanes // QD == a * Y + b, pbuf[a, b], 0)
    subl = lax.broadcasted_iota(jnp.int32, (n_doc, n_query), 0)
    doc_id = (row * 2 * YH * Z + (col // (Z * 2)) * 2 * Z) * DD
    doc_id = doc_id + (subl // DD % Z) * 2 * DD + (subl // (DD * Z)) * DD + subl % DD
    onehot = jnp.where(doc_id == pos, 1.0, 0.0).astype(F32)

    edges = [0] + [width >> m for m in (3, 2, 1, 0)]
    logits = [None] * LEVELS
    running = None
    for s in range(LEVELS):
        first, end = edges[s], edges[s + 1]
        dpart = dbuf[:, :, :, first:end].reshape(n_doc, end - first)
        qpart = qdense[:, :, first:end].reshape(n_query, end - first)
        dots = lax.dot_general(
            dpart, qpart, (((1,), (1,)), ((), ())), preferred_element_type=F32
        )
        running = dots if running is None else running + dots
        logits[LEVELS - 1 - s] = running * (4.0 / math.sqrt(end))
    picked = jnp.zeros((1, n_query), F32)
    for m in range(LEVELS):
        largest = jnp.max(logits[m], axis=0, keepdims=True)
        sy[0, m : m + 1, :] = largest
        sy[0, LEVELS + m : LEVELS + m + 1, :] = jnp.sum(
            jnp.exp(logits[m] - largest), axis=0, keepdims=True
        )
        picked = picked + jnp.sum(onehot * logits[m], axis=0, keepdims=True)
    sy[0, 2 * LEVELS : 2 * LEVELS + 1, :] = picked

    def merged(ref, n):
        tops = [ref[i, 0:LEVELS, :] for i in range(n)]
        top = functools.reduce(jnp.maximum, tops)
        total = sum(ref[i, LEVELS : 2 * LEVELS, :] * jnp.exp(tops[i] - top) for i in range(n))
        return top, total, sum(ref[i, 2 * LEVELS : 2 * LEVELS + 1, :] for i in range(n))

    for o in (4, 3, 5, 2, 6, 1, 7):
        send(sy.at[0], sy.at[o], yo(o), "sy")
    take("sy", sy.at[pl.ds(1, Y - 1)])
    top, total, picked = merged(sy, Y)
    sx[0, 0:LEVELS, :] = top
    sx[0, LEVELS : 2 * LEVELS, :] = total
    sx[0, 2 * LEVELS : 2 * LEVELS + 1, :] = picked
    for o in (2, 1, 3):
        send(sx.at[0], sx.at[o], xo(o), "sx")
    take("sx", sx.at[pl.ds(1, X - 1)])
    top, total, picked = merged(sx, X)
    lse = top + jnp.log(total)

    grads = []
    weighted = None
    for m in range(LEVELS):
        grad = (jnp.exp(logits[m] - lse[m : m + 1, :]) - onehot) * math.sqrt(2.0**m)
        weighted = grad if weighted is None else weighted + grad
        grads.append(weighted)
    for s in range(LEVELS):
        gd = grads[LEVELS - 1 - s].astype(BF)
        for c, n in pieces(edges[s], edges[s + 1]):
            part = jnp.dot(gd, qdense[:, :, c : c + n].reshape(n_query, n), preferred_element_type=F32)
            pd[:, :, c : c + n] = part.astype(BF).reshape(2, Z * DD, n)
    send(pd.at[1 - k], dsib, sib, "sib")
    for s in range(LEVELS):
        gq = grads[LEVELS - 1 - s].T.astype(BF)
        for c, n in pieces(edges[s], edges[s + 1]):
            part = jnp.dot(gq, dbuf[:, :, :, c : c + n].reshape(n_doc, n), preferred_element_type=F32)
            for a in range(X):
                for b in range(Y):
                    at_row = (a * Y + b) * QD
                    block = part[at_row : at_row + QD, :].astype(BF)
                    if c < main:
                        pq[a, b, :, c : c + n] = block
                    else:
                        pqa[b, a, :, c - main : c - main + n] = block

    def a_mine(o, part=None):
        yy = (y + o) % Y
        return pqa.at[yy] if part is None else pqa.at[yy, :, :, part(tail)]

    def a_into(i, part=None):
        return ayr.at[i] if part is None else ayr.at[i, :, :, part(tail)]

    def a_through(i, part=None):
        return ays.at[i] if part is None else ays.at[i, :, :, part(tail)]

    def x_start(o):
        yy = (y + o) % Y
        for dx in (2, 1, 3):
            send(pq.at[(x + dx) % X, yy], xr.at[o, dx - 1], xo(dx), ("x", o))

    def x_finish(o):
        take(("x", o), xr.at[o])
        total = wide(pq[x, (y + o) % Y])
        for i in range(X - 1):
            total = total + wide(xr[o, i])
        if o:
            yp[o] = total.astype(BF)
            send(yp.at[o], yr.at[o], yo(o), "y")
        return total

    x_start(4)
    scatter_start(a_mine, a_into, yo, "ay")
    for o in FAR[1:] + (0,):
        x_start(o)

    lz[0] = jnp.sum(lse, axis=0, keepdims=True) - picked
    for o in NEAR:
        send(lz.at[0], lz.at[o], zo(o), "lz")

    take("sib", dsib)
    for b in range(Z):
        rows = slice(b * DD, (b + 1) * DD)
        zp[b] = (wide(pd[k, rows, :]) + wide(dsib[rows, :])).astype(BF)

    def z_mine(o, part=None):
        zz = (z + o) % Z
        return zp.at[zz] if part is None else zp.at[zz, :, part(width)]

    def z_into(i, part=None):
        return zr.at[i] if part is None else zr.at[i, :, part(width)]

    def z_through(i, part=None):
        return zs.at[i] if part is None else zs.at[i, :, part(width)]

    scatter_start(z_mine, z_into, zo, "z")
    x_finish(4)
    scatter_pass(a_mine, a_into, a_through, yo, "ay")
    x_finish(3)
    x_finish(5)
    x_finish(2)
    x_finish(6)
    x_finish(1)
    x_finish(7)
    scatter_pass(z_mine, z_into, z_through, zo, "z")
    mine = x_finish(0)
    take(("ay", "c"), ayr.at[pl.ds(3, 4)])
    for a in range(X):
        total = wide(pqa[y, a])
        for i in (3, 4, 5, 6):
            total = total + wide(ayr[i, a])
        axp[a] = total.astype(BF)
    for o in (2, 1, 3):
        send(axp.at[(x + o) % X], axr.at[o], xo(o), "ax")
    take("lz", lz.at[pl.ds(1, Z - 1)])
    lk[0] = sum(lz[i] for i in range(Z))
    send(lk.at[0], lk.at[1], sib, "lk")
    take("ax", axr.at[pl.ds(1, X - 1)])
    total = wide(axp[x])
    for o in (1, 2, 3):
        total = total + wide(axr[o])
    dqv[:, main:] = total.astype(BF)
    take("lk", lk.at[1])
    scale = 1.0 / (n_query * 2 * Z * LEVELS)
    total = jnp.sum(lk[0] + lk[1], axis=1, keepdims=True) * scale
    lossv[...] = jnp.broadcast_to(total, (1, n_query))
    puts = [pltpu.make_async_copy(lossv, loss_ref, local.at[0])]
    puts[0].start()
    take(("z", "c"), zr.at[pl.ds(3, 4)])
    ddv[...] = (
        wide(zp[z]) + wide(zr[3]) + wide(zr[4]) + wide(zr[5]) + wide(zr[6])
    ).astype(BF)
    puts.append(pltpu.make_async_copy(ddv, dd_ref, local.at[1]))
    puts[1].start()
    take("y", yr.at[pl.ds(1, Y - 1)])
    for o in NEAR:
        mine = mine + wide(yr[o])
    dqv[:, :main] = mine.astype(BF)
    puts.append(pltpu.make_async_copy(dqv, dq_ref, local.at[2]))
    puts[2].start()
    sent = bulk.at[pl.ds(0, sum(moved) // 512)]
    pltpu.make_async_copy(sent, sent, out_sem).wait()
    for copy in puts:
        copy.wait()


def finish(loss_ref, dq_ref, dd_ref, loss_out, dq_out, dd_out, lossv, dqv, ddv, mean, sems):
    pairs = ((dd_ref, ddv), (dq_ref, dqv), (loss_ref, lossv))
    ins = [pltpu.make_async_copy(a, b, sems.at[i]) for i, (a, b) in enumerate(pairs)]
    pairs = ((ddv, dd_out), (dqv, dq_out), (mean, loss_out))
    outs = [pltpu.make_async_copy(a, b, sems.at[3 + i]) for i, (a, b) in enumerate(pairs)]
    for copy in ins:
        copy.start()
    for i in range(3):
        ins[i].wait()
        if i == 2:
            mean[...] = lossv[:, 0:1]
        outs[i].start()
    for copy in outs:
        copy.wait()


def shards(queries, documents, positive):
    width = queries.shape[1]
    tail = int(width * ALT)
    main = width - tail
    n_query = X * Y * QD
    vm, dma = pltpu.VMEM, pltpu.SemaphoreType.DMA
    stat = 2 * LEVELS + 1
    anywhere = pl.BlockSpec(memory_space=pl.ANY)
    loss, dq, dd = pl.pallas_call(
        kernel,
        out_shape=[
            jax.ShapeDtypeStruct((1, n_query), F32),
            jax.ShapeDtypeStruct(queries.shape, BF),
            jax.ShapeDtypeStruct(documents.shape, BF),
        ],
        in_specs=[anywhere] * 3,
        out_specs=[anywhere] * 3,
        scratch_shapes=[
            vm((X, Y, QD, main), BF),
            vm((Y, X, QD, tail), BF),
            vm((X, Y, 1, n_query), jnp.int32),
            vm((2, Z, DD, width), BF),
            vm((X, Y * QD, width), BF),
            vm((X, Y, QD, main), BF),
            vm((Y, X, QD, tail), BF),
            vm((2, Z * DD, width), BF),
            vm((Y, stat, n_query), F32),
            vm((X, stat, n_query), F32),
            vm((Y, X - 1, QD, main), BF),
            vm((Y, QD, main), BF),
            vm((Y, QD, main), BF),
            vm((7, X, QD, tail), BF),
            vm((2, X, QD, tail), BF),
            vm((X, QD, tail), BF),
            vm((X, QD, tail), BF),
            vm((Z * DD, width), BF),
            vm((Z, DD, width), BF),
            vm((7, DD, width), BF),
            vm((2, DD, width), BF),
            vm((Z, 1, n_query), F32),
            vm((2, 1, n_query), F32),
            vm((1, n_query), F32),
            vm(queries.shape, BF),
            vm(documents.shape, BF),
            pltpu.SMEM((QD,), jnp.int32),
            vm((16384, 128), F32),
            dma((53,)),
            dma,
            dma((4,)),
        ],
        compiler_params=pltpu.CompilerParams(collective_id=0, has_side_effects=True),
    )(queries, documents, positive)
    loss, dq, dd = pl.pallas_call(
        finish,
        out_shape=[
            jax.ShapeDtypeStruct((1, 1), F32),
            jax.ShapeDtypeStruct(queries.shape, BF),
            jax.ShapeDtypeStruct(documents.shape, BF),
        ],
        in_specs=[anywhere] * 3,
        out_specs=[anywhere] * 3,
        scratch_shapes=[
            vm((1, n_query), F32),
            vm(queries.shape, BF),
            vm(documents.shape, BF),
            vm((1, 1), F32),
            dma((6,)),
        ],
    )(loss, dq, dd)
    return (loss.reshape(()), dq, dd)


def solution(mesh):
    placed = (P(("row", "col"), None), P(("row", "col"), None), P(("row", "col")))
    return jax.shard_map(
        shards,
        mesh=mesh,
        in_specs=placed,
        out_specs=(P(), P(("row", "col"), None), P(("row", "col"), None)),
        check_vma=False,
    )
```
